32 devices in a mesh: member: 16 (over z, y, core), slab: 2 (over x).
Axes of the slice: x: 2, y: 2, z: 4, core: 2. Of those that a mesh axis runs over, the one named last changes fastest.
Arguments:
- checkpoint: float32 [16, 2, 4, 256, 256], P('member', None, 'slab'), may hold values from 0 to 1
- adjoint_late: float32 [16, 2, 4, 256, 256], P('member', None, 'slab'), may hold values from -6 to 6
- rate_params: float32 [64, 64], replicated, may hold values from 0.02 to 0.1
- perturbation: float32 [16, 64, 64], P('member'), may hold values from -0.5 to 0.5
Outputs:
- adjoint_early: float32 [16, 2, 4, 256, 256], P('member', None, 'slab')
- param_grad: float32 [64, 64], replicated
The draws below stay inside these ranges and needn't reach their ends.
All inputs are finite; a program needn't handle non-finite values.
Results may differ from the reference program's by a relative error of at most 0.00002.
Values sent between devices are 32-bit elements; how exact they have to be, the bound alone decides.
A program may use at most 64 MiB of HBM per device.

```python
import math
import jax
import jax.numpy as jnp
from jax import lax

PX = 64
PY = 64
SX = 4
SY = 4
MEMBERS = 16
NX = 256
NY = 256
NZ = 4


def levels(own_key, extent, shards, least, top_value):
    def one(axis_at, shards_of):
        draws = jax.random.uniform(jax.random.fold_in(jax.random.fold_in(own_key, 6), axis_at), (shards_of,), jnp.float32, least / len(shards), top_value / len(shards))
        return jnp.repeat(jnp.exp(draws), extent[axis_at] // shards_of).reshape((-1,) + (1,) * (len(extent) - axis_at - 1))

    loudness = one(*shards[0])
    for cut in shards[1:]:
        loudness = loudness * one(*cut)
    return loudness


def normal_values(stream_key, dims, width, bound, split=(), dtype=jnp.bfloat16):
    loudness = levels(stream_key, dims, split, -0.22, 0.18) if split else 1.0
    entries = jax.random.normal(stream_key, dims, jnp.float32) * width * loudness
    return jnp.minimum(jnp.maximum(entries, -bound), bound).astype(dtype)


def setup_inputs(seed: int = 0) -> dict:
    streams_of = jax.random.split(jax.random.key(seed), 5)
    checkpoint = jnp.clip(1.0 * jax.random.uniform(streams_of[0], (MEMBERS, 2, NZ, NX, NY), jnp.float32) ** levels(streams_of[0], (MEMBERS, 2, NZ, NX, NY), ((0, 16), (2, 2)), -0.2, 0.2), 0.0, 1.0)
    adjoint_late = normal_values(streams_of[1], (MEMBERS, 2, NZ, NX, NY), 1.0, 6.0, ((0, 16), (2, 2)), jnp.float32)
    rate_params = jnp.clip(jnp.exp(jax.random.uniform(streams_of[2], (PX, PY), jnp.float32, math.log(0.02), math.log(0.1))), 0.02, 0.1)
    perturbation = jnp.clip(jax.random.uniform(streams_of[3], (MEMBERS, PX, PY), jnp.float32, -0.5, 0.5) * levels(streams_of[3], (MEMBERS, PX, PY), ((0, 16),), -0.4, 0.0), -0.5, 0.5)
    return {"checkpoint": checkpoint, "adjoint_late": adjoint_late, "rate_params": rate_params, "perturbation": perturbation}


feed_rate = 0.035
substrate_diffusion = 0.16
activator_diffusion = 0.08


def laplace_rim(extended):
    padded = jnp.pad(extended, ((0, 0), (0, 0), (1, 1), (1, 1)))
    center = padded[:, 1:-1, 1:-1, 1:-1]
    summed = padded[:, 2:, 1:-1, 1:-1] + padded[:, :-2, 1:-1, 1:-1]
    summed = summed + padded[:, 1:-1, 2:, 1:-1] + padded[:, 1:-1, :-2, 1:-1]
    summed = summed + padded[:, 1:-1, 1:-1, 2:] + padded[:, 1:-1, 1:-1, :-2]
    return summed - 6.0 * center


def advance(extended, decay_rate):
    laplace = laplace_rim(extended)
    u_field = extended[0, 1:-1]
    v_field = extended[1, 1:-1]
    reaction = u_field * v_field * v_field
    u_new = u_field + substrate_diffusion * laplace[0] - reaction + feed_rate * (1.0 - u_field)
    v_new = v_field + activator_diffusion * laplace[1] + reaction - (feed_rate + decay_rate) * v_field
    return jnp.stack([u_new, v_new])


def pull_back(status, adjoint_ext, decay_rate):
    laplace = laplace_rim(adjoint_ext)
    adj_u = adjoint_ext[0, 1:-1]
    adj_v = adjoint_ext[1, 1:-1]
    uv_prod = status[0] * status[1]
    v_square = status[1] * status[1]
    new_u = adj_u + substrate_diffusion * laplace[0] - (v_square + feed_rate) * adj_u + v_square * adj_v
    new_v = adj_v + activator_diffusion * laplace[1] - 2.0 * uv_prod * adj_u + (2.0 * uv_prod - feed_rate - decay_rate) * adj_v
    return jnp.stack([new_u, new_v])


def expand_params(table):
    return jnp.broadcast_to(table[:, None, :, None], (PX, SX, PY, SY)).reshape(NX, NY)


def patch_total(field):
    return jnp.sum(field.reshape(PX, SX, PY, SY), axis=(1, 3))


def pad_planes(field):
    return jnp.pad(field, ((0, 0), (1, 1), (0, 0), (0, 0)))


def reference(checkpoint, adjoint_late, rate_params, perturbation):
    def one_member(member_item):
        start_state, adjoint_two, member_shift = member_item
        factor = 1.0 + member_shift
        decay_rate = expand_params(rate_params * factor)
        middle = advance(pad_planes(start_state), decay_rate)
        adjoint_one = pull_back(middle, pad_planes(adjoint_two), decay_rate)
        adjoint_zero = pull_back(start_state, pad_planes(adjoint_one), decay_rate)
        cell_grad = -(jnp.sum(middle[1] * adjoint_two[1], 0) + jnp.sum(start_state[1] * adjoint_one[1], 0))
        return adjoint_zero, patch_total(cell_grad) * factor

    adjoint_early, grads = lax.map(one_member, (checkpoint, adjoint_late, perturbation))
    return adjoint_early, jnp.sum(grads, 0) / MEMBERS
```

```python
import functools

import jax
import jax.numpy as jnp
from jax import lax
from jax.experimental import pallas as pl
from jax.experimental.pallas import tpu as pltpu
from jax.sharding import PartitionSpec as P

MESH = pl.DeviceIdType.MESH
HIGH = lax.Precision.HIGHEST
PAD = 8
ROWS = 16
CHUNKS = 4

feed_rate = 0.035
substrate_diffusion = 0.16
activator_diffusion = 0.08


def bits_of(count):
    return [1 << i for i in range((count - 1).bit_length())]


def spread(rows, cols):
    r = lax.broadcasted_iota(jnp.int32, (rows, cols), 0)
    c = lax.broadcasted_iota(jnp.int32, (rows, cols), 1)
    if rows >= cols:
        size = rows // cols
        hit = (r >= c * size) & (r < (c + 1) * size)
    else:
        size = cols // rows
        hit = (c >= r * size) & (c < (r + 1) * size)
    return hit.astype(jnp.float32)


def dot(a, b):
    return jnp.dot(a, b, precision=HIGH, preferred_element_type=jnp.float32)


def kernel(
    n, members, ck_hbm, la_hbm, rate_ref, pert_ref, out_hbm, grad_ref,
    ck, la, mi, ob, decay, cell, gbuf, gsum,
    local_sem, in_send, in_recv, mid_send, mid_recv, g_send, g_recv, out_sem,
):
    nz, nx, ny = ob.shape[1], ob.shape[2], ob.shape[3]
    px, py = rate_ref.shape
    chunk = nx // CHUNKS
    idx = lax.axis_index("slab")
    mem = lax.axis_index("member")
    partners = [("slab", lax.bitwise_xor(idx, b)) for b in bits_of(n)]
    partners += [("member", lax.bitwise_xor(mem, b)) for b in bits_of(members)]
    has = {0: idx > 0, 1: idx < n - 1}
    peer = {0: idx - 1, 1: idx + 1}
    halo = {0: 0, 1: nz + 1}
    edge = {0: nz, 1: 1}

    loads = [
        pltpu.make_async_copy(src.at[0], dst.at[:, pl.ds(1, nz), pl.ds(PAD, nx), :], local_sem.at[i])
        for i, (src, dst) in enumerate(((ck_hbm, ck), (la_hbm, la)))
    ]
    for load in loads:
        load.start()

    barrier = pltpu.get_barrier_semaphore()
    greeted = [("slab", lax.rem(idx + j, n)) for j in range(1, n)]
    greeted += [p for p in partners if p[0] == "member"]
    for axis, who in greeted:
        pl.semaphore_signal(barrier, inc=1, device_id={axis: who}, device_id_type=MESH)
    pl.semaphore_wait(barrier, len(greeted))

    def in_copy(side, c, which):
        src, dst = ((ck_hbm, ck), (la_hbm, la))[which]
        return pltpu.make_async_remote_copy(
            src_ref=src.at[0, :, edge[side] - 1, pl.ds(c * chunk, chunk), :],
            dst_ref=dst.at[:, halo[side], pl.ds(PAD + c * chunk, chunk), :],
            send_sem=in_send.at[side, c, which],
            recv_sem=in_recv.at[side, c, which],
            device_id={"slab": peer[1 - side]},
            device_id_type=MESH,
        )

    def mid_copy(side, c):
        return pltpu.make_async_remote_copy(
            src_ref=mi.at[:, edge[side], pl.ds(PAD + c * chunk, chunk), :],
            dst_ref=mi.at[:, halo[side], pl.ds(PAD + c * chunk, chunk), :],
            send_sem=mid_send.at[side, c],
            recv_sem=mid_recv.at[side, c],
            device_id={"slab": peer[1 - side]},
            device_id_type=MESH,
        )

    def on_send(do):
        for side in (0, 1):
            @pl.when(has[1 - side])
            def _(side=side):
                do(side)

    def on_recv(do):
        for side in (0, 1):
            @pl.when(has[side])
            def _(side=side):
                do(side)

    for c in range(CHUNKS):
        for which in (0, 1):
            on_send(lambda side: in_copy(side, c, which).start())

    zero_rows = jnp.zeros((2, nz, PAD, ny), jnp.float32)
    for ref in (ck, la, mi):
        ref[:, 1 : nz + 1, 0:PAD, :] = zero_rows
        ref[:, 1 : nz + 1, PAD + nx : 2 * PAD + nx, :] = zero_rows
    for side in (0, 1):
        @pl.when(jnp.logical_not(has[side]))
        def _(side=side):
            zero = jnp.zeros((2, 2 * PAD + nx, ny), jnp.float32)
            ck[:, halo[side]] = zero
            la[:, halo[side]] = zero

    factor = 1.0 + pert_ref[0]
    decay[...] = dot(dot(spread(nx, px), rate_ref[...] * factor), spread(py, ny))
    for load in loads:
        load.wait()

    col = lax.broadcasted_iota(jnp.int32, (ROWS, ny), 1)
    first, last = col == 0, col == ny - 1

    def ring(ref, s, z, r):
        x = ref[s, z, pl.ds(r, ROWS + 2 * PAD), :]
        c = x[PAD : PAD + ROWS]
        total = x[PAD - 1 : PAD - 1 + ROWS] + x[PAD + 1 : PAD + 1 + ROWS]
        total = total + jnp.where(first, 0.0, pltpu.roll(c, 1, 1))
        total = total + jnp.where(last, 0.0, pltpu.roll(c, ny - 1, 1))
        return c, total

    def rows_of(ref, s, z, r):
        return ref[s, z, pl.ds(r + PAD, ROWS), :]

    def laplace(ref, s, z, r, low, high):
        c, total = ring(ref, s, z, r)
        if low:
            total = total + rows_of(ref, s, z - 1, r)
        if high:
            total = total + rows_of(ref, s, z + 1, r)
        return c, total - 6.0 * c

    def pull(um, vm, a, b, la_a, la_b, k):
        v2 = vm * vm
        uv2 = 2.0 * (um * vm)
        new_a = a + substrate_diffusion * la_a - (v2 + feed_rate) * a + v2 * b
        new_b = b + activator_diffusion * la_b - uv2 * a + (uv2 - feed_rate - k) * b
        return new_a, new_b

    def mid_block(r):
        k = decay[pl.ds(r, ROWS), :]
        g = None
        for z in range(1, nz + 1):
            u, lu = laplace(ck, 0, z, r, True, True)
            v, lv = laplace(ck, 1, z, r, True, True)
            react = u * v * v
            um = u + substrate_diffusion * lu - react + feed_rate * (1.0 - u)
            vm = v + activator_diffusion * lv + react - (feed_rate + k) * v
            a, l_a = laplace(la, 0, z, r, True, True)
            b, l_b = laplace(la, 1, z, r, True, True)
            new_a, new_b = pull(um, vm, a, b, l_a, l_b, k)
            mi[0, z, pl.ds(r + PAD, ROWS), :] = new_a
            mi[1, z, pl.ds(r + PAD, ROWS), :] = new_b
            term = vm * b + v * new_b
            g = term if g is None else g + term
        cell[pl.ds(r, ROWS), :] = g

    def early_block(r):
        k = decay[pl.ds(r, ROWS), :]
        for z in range(1, nz + 1):
            u, v = rows_of(ck, 0, z, r), rows_of(ck, 1, z, r)
            a, l_a = laplace(mi, 0, z, r, z > 1, z < nz)
            b, l_b = laplace(mi, 1, z, r, z > 1, z < nz)
            new_a, new_b = pull(u, v, a, b, l_a, l_b, k)
            ob[0, z - 1, pl.ds(r, ROWS), :] = new_a
            ob[1, z - 1, pl.ds(r, ROWS), :] = new_b

    def blocks(c, body):
        def step(i, carry):
            body(pl.multiple_of(c * chunk + i * ROWS, ROWS))
            return carry

        lax.fori_loop(0, chunk // ROWS, step, 0)

    for c in range(CHUNKS):
        for which in (0, 1):
            on_recv(lambda side: in_copy(side, c, which).wait_recv())
        blocks(c, mid_block)
        if c == 0:
            on_send(lambda side: mid_copy(side, 0).start())

    total = dot(dot(spread(px, nx), cell[...]), spread(ny, py))
    gsum[0] = total * factor * (-1.0 / members)

    def g_copy(i):
        axis, who = partners[i]
        return pltpu.make_async_remote_copy(
            src_ref=gsum.at[i],
            dst_ref=gbuf.at[i],
            send_sem=g_send.at[i],
            recv_sem=g_recv.at[i],
            device_id={axis: who},
            device_id_type=MESH,
        )

    if partners:
        g_copy(0).start()
    for c in range(1, CHUNKS):
        on_send(lambda side: mid_copy(side, c).start())

    steps = max(CHUNKS, len(partners))
    for i in range(steps):
        if i < CHUNKS:
            blocks(i, early_block)
        if i < len(partners):
            g_copy(i).wait_recv()
            gsum[i + 1] = gsum[i] + gbuf[i]
            if i + 1 < len(partners):
                g_copy(i + 1).start()
    grad_ref[...] = gsum[len(partners)]

    def out_copy(c):
        rows = pl.ds(c * chunk, chunk)
        return pltpu.make_async_copy(ob.at[:, :, rows, :], out_hbm.at[0, :, :, rows, :], out_sem.at[c])

    scales = (substrate_diffusion, activator_diffusion)
    for c in range(CHUNKS):
        def add(side):
            mid_copy(side, c).wait_recv()
            for s in (0, 1):
                ob[s, (0, nz - 1)[side], pl.ds(c * chunk, chunk), :] += (
                    scales[s] * mi[s, halo[side], pl.ds(PAD + c * chunk, chunk), :]
                )

        on_recv(add)
        out_copy(c).start()

    for c in range(CHUNKS):
        for which in (0, 1):
            on_send(lambda side: in_copy(side, c, which).wait_send())
        on_send(lambda side: mid_copy(side, c).wait_send())
        out_copy(c).wait()
    for i in range(len(partners)):
        g_copy(i).wait_send()


def solution(mesh):
    n, members = mesh.shape["slab"], mesh.shape["member"]
    count = len(bits_of(n)) + len(bits_of(members))

    def local(checkpoint, adjoint_late, rate_params, perturbation):
        _, _, nz, nx, ny = checkpoint.shape
        px, py = rate_params.shape
        f32 = jnp.float32
        field = pltpu.VMEM((2, nz + 2, nx + 2 * PAD, ny), f32)
        dma = pltpu.SemaphoreType.DMA
        return pl.pallas_call(
            functools.partial(kernel, n, members),
            out_shape=(
                jax.ShapeDtypeStruct(checkpoint.shape, f32),
                jax.ShapeDtypeStruct((px, py), f32),
            ),
            in_specs=[
                pl.BlockSpec(memory_space=pl.ANY),
                pl.BlockSpec(memory_space=pl.ANY),
                pl.BlockSpec(memory_space=pltpu.VMEM),
                pl.BlockSpec(memory_space=pltpu.VMEM),
            ],
            out_specs=(
                pl.BlockSpec(memory_space=pl.ANY),
                pl.BlockSpec(memory_space=pltpu.VMEM),
            ),
            scratch_shapes=[
                field,
                field,
                field,
                pltpu.VMEM((2, nz, nx, ny), f32),
                pltpu.VMEM((nx, ny), f32),
                pltpu.VMEM((nx, ny), f32),
                pltpu.VMEM((count, px, py), f32),
                pltpu.VMEM((count + 1, px, py), f32),
                dma((2,)),
                dma((2, CHUNKS, 2)),
                dma((2, CHUNKS, 2)),
                dma((2, CHUNKS)),
                dma((2, CHUNKS)),
                dma((count,)),
                dma((count,)),
                dma((CHUNKS,)),
            ],
            compiler_params=pltpu.CompilerParams(collective_id=0, has_side_effects=True),
        )(checkpoint, adjoint_late, rate_params, perturbation)

    return jax.shard_map(
        local,
        mesh=mesh,
        in_specs=(
            P("member", None, "slab", None, None),
            P("member", None, "slab", None, None),
            P(),
            P("member", None, None),
        ),
        out_specs=(P("member", None, "slab", None, None), P()),
        check_vma=False,
    )
```

```python
import functools

import jax
import jax.numpy as jnp
from jax import lax
from jax.experimental import pallas as pl
from jax.experimental.pallas import tpu as pltpu
from jax.sharding import PartitionSpec as P

MESH = pl.DeviceIdType.MESH
HIGH = lax.Precision.HIGHEST
PAD = 8
ROWS = 16
CHUNKS = 8

feed_rate = 0.035
substrate_diffusion = 0.16
activator_diffusion = 0.08


def stages_of(n, members):
    stages, slot = [], 0
    for axis, count in (("member", members), ("slab", n)):
        bit = 1
        while bit < count:
            radix = 4 if bit * 4 <= count else 2
            stages.append((axis, [bit * j for j in range(1, radix)], slot))
            bit, slot = bit * radix, slot + radix - 1
    return stages, slot


def spread(rows, cols):
    r = lax.broadcasted_iota(jnp.int32, (rows, cols), 0)
    c = lax.broadcasted_iota(jnp.int32, (rows, cols), 1)
    if rows >= cols:
        size = rows // cols
        hit = (r >= c * size) & (r < (c + 1) * size)
    else:
        size = cols // rows
        hit = (c >= r * size) & (c < (r + 1) * size)
    return hit.astype(jnp.float32)


def dot(a, b):
    return jnp.dot(a, b, precision=HIGH, preferred_element_type=jnp.float32)


def kernel(
    n, members, ck_hbm, la_hbm, rate_ref, pert_ref, out_hbm, grad_ref,
    ck, la, mi, ob, decay, weight, cell, gbuf, gsum,
    local_sem, in_send, in_recv, mid_send, mid_recv, g_send, g_recv, out_sem,
):
    nz, nx, ny = ob.shape[1], ob.shape[2], ob.shape[3]
    px, py = rate_ref.shape
    chunk = nx // CHUNKS
    idx = lax.axis_index("slab")
    mem = lax.axis_index("member")
    stages, _ = stages_of(n, members)
    has = {0: idx > 0, 1: idx < n - 1}
    peer = {0: idx - 1, 1: idx + 1}
    halo = {0: 0, 1: nz + 1}
    edge = {0: nz, 1: 1}

    loads = [
        pltpu.make_async_copy(src.at[0], dst.at[:, pl.ds(1, nz), pl.ds(PAD, nx), :], local_sem.at[i])
        for i, (src, dst) in enumerate(((ck_hbm, ck), (la_hbm, la)))
    ]
    for load in loads:
        load.start()

    barrier = pltpu.get_barrier_semaphore()
    greeted = [("slab", lax.rem(idx + j, n)) for j in range(1, n)]
    for axis, offsets, _ in stages:
        if axis == "member":
            greeted += [(axis, lax.bitwise_xor(mem, j)) for j in offsets]
    for axis, who in greeted:
        pl.semaphore_signal(barrier, inc=1, device_id={axis: who}, device_id_type=MESH)
    pl.semaphore_wait(barrier, len(greeted))

    def in_copy(side, c, which):
        src, dst = ((ck_hbm, ck), (la_hbm, la))[which]
        return pltpu.make_async_remote_copy(
            src_ref=src.at[0, :, edge[side] - 1, pl.ds(c * chunk, chunk), :],
            dst_ref=dst.at[:, halo[side], pl.ds(PAD + c * chunk, chunk), :],
            send_sem=in_send.at[side, c, which],
            recv_sem=in_recv.at[side, c, which],
            device_id={"slab": peer[1 - side]},
            device_id_type=MESH,
        )

    def mid_copy(side, c):
        return pltpu.make_async_remote_copy(
            src_ref=mi.at[:, edge[side], pl.ds(PAD + c * chunk, chunk), :],
            dst_ref=mi.at[:, halo[side], pl.ds(PAD + c * chunk, chunk), :],
            send_sem=mid_send.at[side, c],
            recv_sem=mid_recv.at[side, c],
            device_id={"slab": peer[1 - side]},
            device_id_type=MESH,
        )

    def on_send(do):
        for side in (0, 1):
            @pl.when(has[1 - side])
            def _(side=side):
                do(side)

    def on_recv(do):
        for side in (0, 1):
            @pl.when(has[side])
            def _(side=side):
                do(side)

    for c in range(CHUNKS):
        for which in (0, 1):
            on_send(lambda side: in_copy(side, c, which).start())

    zero_rows = jnp.zeros((2, nz, PAD, ny), jnp.float32)
    for ref in (ck, la, mi):
        ref[:, 1 : nz + 1, 0:PAD, :] = zero_rows
        ref[:, 1 : nz + 1, PAD + nx : 2 * PAD + nx, :] = zero_rows
    for side in (0, 1):
        @pl.when(jnp.logical_not(has[side]))
        def _(side=side):
            zero = jnp.zeros((2, 2 * PAD + nx, ny), jnp.float32)
            ck[:, halo[side]] = zero
            la[:, halo[side]] = zero

    factor = 1.0 + pert_ref[0]
    weight[...] = dot(dot(spread(nx, px), factor * (-1.0 / members)), spread(py, ny))
    decay[...] = dot(dot(spread(nx, px), rate_ref[...] * factor), spread(py, ny))
    for load in loads:
        load.wait()

    col = lax.broadcasted_iota(jnp.int32, (ROWS, ny), 1)
    first, last = col == 0, col == ny - 1

    def ring(ref, s, z, r):
        x = ref[s, z, pl.ds(r, ROWS + 2 * PAD), :]
        c = x[PAD : PAD + ROWS]
        total = x[PAD - 1 : PAD - 1 + ROWS] + x[PAD + 1 : PAD + 1 + ROWS]
        total = total + jnp.where(first, 0.0, pltpu.roll(c, 1, 1))
        total = total + jnp.where(last, 0.0, pltpu.roll(c, ny - 1, 1))
        return c, total

    def rows_of(ref, s, z, r):
        return ref[s, z, pl.ds(r + PAD, ROWS), :]

    def laplace(ref, s, z, r, low, high):
        c, total = ring(ref, s, z, r)
        if low:
            total = total + rows_of(ref, s, z - 1, r)
        if high:
            total = total + rows_of(ref, s, z + 1, r)
        return c, total - 6.0 * c

    def pull(um, vm, a, b, la_a, la_b, k):
        v2 = vm * vm
        uv2 = 2.0 * (um * vm)
        new_a = a + substrate_diffusion * la_a - (v2 + feed_rate) * a + v2 * b
        new_b = b + activator_diffusion * la_b - uv2 * a + (uv2 - feed_rate - k) * b
        return new_a, new_b

    def mid_block(r):
        k = decay[pl.ds(r, ROWS), :]
        g = None
        for z in range(1, nz + 1):
            u, lu = laplace(ck, 0, z, r, True, True)
            v, lv = laplace(ck, 1, z, r, True, True)
            react = u * v * v
            um = u + substrate_diffusion * lu - react + feed_rate * (1.0 - u)
            vm = v + activator_diffusion * lv + react - (feed_rate + k) * v
            a, l_a = laplace(la, 0, z, r, True, True)
            b, l_b = laplace(la, 1, z, r, True, True)
            new_a, new_b = pull(um, vm, a, b, l_a, l_b, k)
            mi[0, z, pl.ds(r + PAD, ROWS), :] = new_a
            mi[1, z, pl.ds(r + PAD, ROWS), :] = new_b
            term = vm * b + v * new_b
            g = term if g is None else g + term
        cell[pl.ds(r, ROWS), :] = g * weight[pl.ds(r, ROWS), :]

    def early_block(r):
        k = decay[pl.ds(r, ROWS), :]
        for z in range(1, nz + 1):
            u, v = rows_of(ck, 0, z, r), rows_of(ck, 1, z, r)
            a, l_a = laplace(mi, 0, z, r, z > 1, z < nz)
            b, l_b = laplace(mi, 1, z, r, z > 1, z < nz)
            new_a, new_b = pull(u, v, a, b, l_a, l_b, k)
            ob[0, z - 1, pl.ds(r, ROWS), :] = new_a
            ob[1, z - 1, pl.ds(r, ROWS), :] = new_b

    def blocks(c, body):
        def step(i, carry):
            body(pl.multiple_of(c * chunk + i * ROWS, ROWS))
            return carry

        lax.fori_loop(0, chunk // ROWS, step, 0)

    patch_rows = px // CHUNKS
    half = patch_rows // 2

    def packed_sums(c):
        sums = dot(spread(patch_rows, chunk), cell[pl.ds(c * chunk, chunk), :])
        size = ny // py
        r = lax.broadcasted_iota(jnp.int32, (ny, 2 * py), 0)
        q = lax.broadcasted_iota(jnp.int32, (ny, 2 * py), 1) * size
        upper = ((r >= q) & (r < q + size)).astype(jnp.float32)
        lower = ((r + ny >= q) & (r + ny < q + size)).astype(jnp.float32)
        return dot(sums[:half], upper) + dot(sums[half:], lower)

    def g_copies(s):
        axis, offsets, slot = stages[s]
        own = mem if axis == "member" else idx
        return [
            pltpu.make_async_remote_copy(
                src_ref=gsum.at[s],
                dst_ref=gbuf.at[slot + j],
                send_sem=g_send.at[slot + j],
                recv_sem=g_recv.at[slot + j],
                device_id={axis: lax.bitwise_xor(own, offset)},
                device_id_type=MESH,
            )
            for j, offset in enumerate(offsets)
        ]

    def add_up(s):
        _, offsets, slot = stages[s]
        for copy in g_copies(s):
            copy.wait_recv()
        value = gsum[s] + gbuf[slot]
        if len(offsets) == 3:
            value = value + (gbuf[slot + 1] + gbuf[slot + 2])
        gsum[s + 1] = value

    for c in range(CHUNKS):
        for which in (0, 1):
            on_recv(lambda side: in_copy(side, c, which).wait_recv())
        blocks(c, mid_block)
        gsum[0, pl.ds(c * half, half), :] = packed_sums(c)
        if c == 0:
            on_send(lambda side: mid_copy(side, 0).start())

    sent, early = 1, 0
    for s in range(max(len(stages), 1)):
        if s > 0:
            add_up(s - 1)
        if s < len(stages):
            for copy in g_copies(s):
                copy.start()
        upto = CHUNKS if s >= len(stages) - 1 else 1 + (CHUNKS - 1) * (s + 1) // max(len(stages), 1)
        for c in range(sent, upto):
            on_send(lambda side: mid_copy(side, c).start())
        sent = max(sent, upto)
        upto = CHUNKS if s >= len(stages) - 1 else CHUNKS * (s + 1) // len(stages)
        for c in range(early, upto):
            blocks(c, early_block)
        early = max(early, upto)
    def out_copy(c):
        rows = pl.ds(c * chunk, chunk)
        return pltpu.make_async_copy(ob.at[:, :, rows, :], out_hbm.at[0, :, :, rows, :], out_sem.at[c])

    scales = (substrate_diffusion, activator_diffusion)
    for c in range(CHUNKS):
        def add(side):
            mid_copy(side, c).wait_recv()
            for s in (0, 1):
                ob[s, (0, nz - 1)[side], pl.ds(c * chunk, chunk), :] += (
                    scales[s] * mi[s, halo[side], pl.ds(PAD + c * chunk, chunk), :]
                )

        on_recv(add)
        out_copy(c).start()

    if stages:
        add_up(len(stages) - 1)
    for c in range(CHUNKS):
        value = gsum[len(stages), pl.ds(c * half, half), :]
        grad_ref[pl.ds(c * patch_rows, half), :] = value[:, :py]
        grad_ref[pl.ds(c * patch_rows + half, half), :] = pltpu.roll(value, py, 1)[:, :py]

    for c in range(CHUNKS):
        for which in (0, 1):
            on_send(lambda side: in_copy(side, c, which).wait_send())
        on_send(lambda side: mid_copy(side, c).wait_send())
        out_copy(c).wait()
    for s in range(len(stages)):
        for copy in g_copies(s):
            copy.wait_send()


def solution(mesh):
    n, members = mesh.shape["slab"], mesh.shape["member"]
    stages, slots = stages_of(n, members)

    def local(checkpoint, adjoint_late, rate_params, perturbation):
        _, _, nz, nx, ny = checkpoint.shape
        px, py = rate_params.shape
        f32 = jnp.float32
        field = pltpu.VMEM((2, nz + 2, nx + 2 * PAD, ny), f32)
        dma = pltpu.SemaphoreType.DMA
        return pl.pallas_call(
            functools.partial(kernel, n, members),
            out_shape=(
                jax.ShapeDtypeStruct(checkpoint.shape, f32),
                jax.ShapeDtypeStruct((px, py), f32),
            ),
            in_specs=[
                pl.BlockSpec(memory_space=pl.ANY),
                pl.BlockSpec(memory_space=pl.ANY),
                pl.BlockSpec(memory_space=pltpu.VMEM),
                pl.BlockSpec(memory_space=pltpu.VMEM),
            ],
            out_specs=(
                pl.BlockSpec(memory_space=pl.ANY),
                pl.BlockSpec(memory_space=pltpu.VMEM),
            ),
            scratch_shapes=[
                field,
                field,
                field,
                pltpu.VMEM((2, nz, nx, ny), f32),
                pltpu.VMEM((nx, ny), f32),
                pltpu.VMEM((nx, ny), f32),
                pltpu.VMEM((nx, ny), f32),
                pltpu.VMEM((slots, px // 2, 2 * py), f32),
                pltpu.VMEM((len(stages) + 1, px // 2, 2 * py), f32),
                dma((2,)),
                dma((2, CHUNKS, 2)),
                dma((2, CHUNKS, 2)),
                dma((2, CHUNKS)),
                dma((2, CHUNKS)),
                dma((slots,)),
                dma((slots,)),
                dma((CHUNKS,)),
            ],
            compiler_params=pltpu.CompilerParams(collective_id=0, has_side_effects=True),
        )(checkpoint, adjoint_late, rate_params, perturbation)

    return jax.shard_map(
        local,
        mesh=mesh,
        in_specs=(
            P("member", None, "slab", None, None),
            P("member", None, "slab", None, None),
            P(),
            P("member", None, None),
        ),
        out_specs=(P("member", None, "slab", None, None), P()),
        check_vma=False,
    )
```
